32 devices in a mesh: bank: 16 (over z, x, core), zero: 2 (over y).
Axes of the slice: x: 2, y: 2, z: 4, core: 2. Of those that a mesh axis runs over, the one named last changes fastest.
Arguments:
- master_down: float32 [64, 1408, 2048], P('bank', None, 'zero'), may hold values from -0.21875 to 0.21875
- second_down: bfloat16 [64, 1408, 2048], P('bank', None, 'zero'), may hold values from -0.078125 to 0.078125
- router_weight: float32 [2048, 64], P('zero', 'bank'), may hold values from -0.125 to 0.125
- router_gain: float32 [2048], P('zero'), may hold values from 0.25 to 1.75
Outputs:
- final_down: bfloat16 [64, 1408, 2048], P('bank')
- scale_down: float32 [64, 1408], P('bank')
- serve_router: bfloat16 [2048, 64], replicated
The draws below stay inside these ranges and needn't reach their ends.
All inputs are finite; a program needn't handle non-finite values.
Results may differ from the reference program's by a relative error of at most 0.001.
Values may be sent and summed in bfloat16 or wider, within the bound.
No kernel may reach another device: no remote copies, remote signals or barrier semaphores. Data moves between devices by JAX's collectives and lax.ppermute only.
A program may use at most 128 MiB of HBM per device.

```python
import jax
import jax.numpy as jnp
from jax import lax

EXPERTS = 64
D_MODEL = 2048
D_EXPERT = 1408


def with_spikes(result, own_key, source, target, shards_of, factor):
    owner, partner = [(jnp.arange(result.shape[axis_at]) // (result.shape[axis_at] // shards_of)).reshape([-1 if axis == axis_at else 1 for axis in range(result.ndim)]) for axis_at in (source, target)]
    chosen = jax.random.permutation(own_key, shards_of)[partner]
    strong = (owner == chosen) | (owner == (partner + shards_of // 2) % shards_of)
    return jnp.where(strong, factor * result, result)


def level_of(key, shape, pieces, low, top_value):
    def one(dim, parts):
        draws = jax.random.uniform(jax.random.fold_in(jax.random.fold_in(key, 6), dim), (parts,), jnp.float32, low / len(pieces), top_value / len(pieces))
        return jnp.repeat(jnp.exp(draws), shape[dim] // parts).reshape((-1,) + (1,) * (len(shape) - dim - 1))

    level = one(*pieces[0])
    for cut in pieces[1:]:
        level = level * one(*cut)
    return level


def centred(rng, dims, deviation, most, shards=(), dtype=jnp.bfloat16):
    entries = deviation * jax.random.normal(rng, dims, jnp.float32)
    if shards:
        entries = entries * level_of(rng, dims, shards, -0.22, 0.18)
    return jnp.clip(entries, -most, most).astype(dtype)


def noise_with(own_key, shape, scale, bound, shards, heavy, kind=jnp.bfloat16):
    array = scale * jax.random.normal(own_key, shape, jnp.float32)
    if shards:
        array = array * level_of(own_key, shape, shards, -0.22, 0.18)
    return jnp.clip(with_spikes(array, jax.random.fold_in(own_key, 3), *heavy), -bound, bound).astype(kind)


def setup_inputs(seed: int = 0) -> dict:
    keys = jax.random.split(jax.random.key(seed), 5)
    return {
        "master_down": noise_with(keys[0], (EXPERTS, D_EXPERT, D_MODEL), D_EXPERT ** -0.5, 0.21875, ((0, 16), (2, 2)), (2, 1, 2, 2.0), jnp.float32),
        "second_down": centred(keys[1], (EXPERTS, D_EXPERT, D_MODEL), (D_EXPERT * 4) ** -0.5, 0.078125, ((0, 16), (2, 2))),
        "router_weight": centred(keys[2], (D_MODEL, EXPERTS), D_MODEL ** -0.5, 0.125, ((0, 2), (1, 16)), jnp.float32),
        "router_gain": jnp.clip(1.0 + 0.15 * jax.random.normal(keys[3], (D_MODEL,), jnp.float32), 0.25, 1.75),
    }


def reference(master_down, second_down, router_weight, router_gain):
    merged_down = master_down + second_down.astype(jnp.float32)
    scale_down = jnp.sqrt(lax.optimization_barrier(jnp.sum(merged_down * merged_down, axis=2)))
    final_down = (merged_down / jnp.expand_dims(scale_down, 2)).astype(jnp.bfloat16)
    serve_router = (router_weight * router_gain[:, None]).astype(jnp.bfloat16)
    return (final_down, scale_down, serve_router)
```

```python
import functools

import jax
import jax.numpy as jnp
from jax import lax
from jax.experimental import pallas as pl
from jax.experimental.pallas import tpu as pltpu
from jax.sharding import PartitionSpec as P


LANES = 128
PAIR = ((0, 1), (1, 0))


def cost(us):
    return pl.CostEstimate(flops=int(us * 1e6), bytes_accessed=1024, transcendentals=0)


def params():
    return pltpu.CompilerParams(vmem_limit_bytes=16 * 1024 * 1024)


def tile(m_ref, s_ref, b, k):
    rows, cols = pl.ds(b * LANES, LANES), pl.ds(k * LANES, LANES)
    return m_ref[rows, cols] + s_ref[rows, cols].astype(jnp.float32)


def sums_kernel(m_ref, s_ref, *refs):
    sums_ref = refs[-1]
    for b in range(m_ref.shape[0] // LANES):
        acc = jnp.zeros((LANES, LANES), jnp.float32)
        for k in range(m_ref.shape[1] // LANES):
            v = tile(m_ref, s_ref, b, k)
            acc = acc + v * v
        sums_ref[b] = jnp.sum(acc.T, axis=0, keepdims=True)


def norm_kernel(m_ref, s_ref, own_ref, other_ref, *refs):
    send_ref, out_ref = refs[-2:]
    for b in range(m_ref.shape[0] // LANES):
        inverse = 1.0 / jnp.sqrt(own_ref[b] + other_ref[b])
        inverse = jnp.broadcast_to(inverse, (LANES, LANES)).T
        rows = pl.ds(b * LANES, LANES)
        for k in range(m_ref.shape[1] // LANES):
            cols = pl.ds(k * LANES, LANES)
            r = (tile(m_ref, s_ref, b, k) * inverse).astype(jnp.bfloat16)
            send_ref[rows, cols] = r
            out_ref[rows, cols] = r


def place_kernel(row, recv_ref, _, out_ref, sem):
    rows, width = recv_ref.shape
    side = pl.multiple_of((1 - lax.axis_index("zero")) * width, LANES)
    copy = pltpu.make_async_copy(recv_ref, out_ref.at[pl.ds(row, rows), pl.ds(side, width)], sem)
    copy.start()
    copy.wait()


def step_rows(first, count):
    for rows in (512, 256):
        if first % rows == 0 and count % rows == 0:
            return rows
    return LANES


def in_hbm(x):
    return pltpu.with_memory_space_constraint(x, pltpu.HBM)


def sums_of(m, s, first, count, after=None):
    rows, width = step_rows(first, count), m.shape[1]
    at = first // rows
    block = pl.BlockSpec((rows, width), lambda i: (at + i, 0))
    held = [] if after is None else [after]
    return pl.pallas_call(
        sums_kernel,
        grid=(count // rows,),
        in_specs=[block, block] + [pl.BlockSpec(memory_space=pl.ANY)] * len(held),
        out_specs=pl.BlockSpec((rows // LANES, 1, LANES), lambda i: (i, 0, 0)),
        out_shape=jax.ShapeDtypeStruct((count // LANES, 1, LANES), jnp.float32),
        compiler_params=params(),
        cost_estimate=cost(count * 0.002),
        name="sums",
    )(m, s, *held)


def norm_of(m, s, own, other, base, first, count, out):
    rows, width = min(step_rows(first, count), step_rows(first - base, count)), m.shape[1]
    at, near = first // rows, (first - base) // rows
    block = pl.BlockSpec((rows, width), lambda i: (at + i, 0))
    sums = pl.BlockSpec((rows // LANES, 1, LANES), lambda i: (near + i, 0, 0))
    whole = jax.ShapeDtypeStruct((m.shape[0], 2 * width), jnp.bfloat16)
    held = [] if out is None else [out]
    return pl.pallas_call(
        norm_kernel,
        grid=(count // rows,),
        in_specs=[block, block, sums, sums] + [pl.BlockSpec(memory_space=pl.ANY)] * len(held),
        out_specs=[
            pl.BlockSpec((rows, width), lambda i: (i, 0)),
            pl.BlockSpec((rows, width), lambda i: (at + i, lax.axis_index("zero"))),
        ],
        out_shape=[jax.ShapeDtypeStruct((count, width), jnp.bfloat16), whole],
        input_output_aliases={4: 1} if held else {},
        compiler_params=params(),
        cost_estimate=cost(count * 0.003),
        name="norm",
    )(m, s, own, other, *held)


def place(recv, out, row):
    return pl.pallas_call(
        functools.partial(place_kernel, row),
        in_specs=[pl.BlockSpec(memory_space=pltpu.VMEM), pl.BlockSpec(memory_space=pl.ANY)],
        out_specs=pl.BlockSpec(memory_space=pl.ANY),
        out_shape=jax.ShapeDtypeStruct(out.shape, out.dtype),
        scratch_shapes=[pltpu.SemaphoreType.DMA],
        input_output_aliases={1: 0},
        compiler_params=params(),
        cost_estimate=cost(1),
        name="place",
    )(recv, out)


def swap(x):
    return lax.ppermute(x, "zero", PAIR)


def cuts(blocks):
    sizes = [2]
    blocks -= 2
    while blocks > 8:
        sizes.append(8)
        blocks -= 8
    while blocks > 1:
        sizes.append(blocks // 2)
        blocks -= blocks // 2
    return sizes + [1]


HEAD = (3, 1)


def pair_body(master_down, second_down, router_weight, router_gain):
    return pair_steps(master_down, second_down, router_weight, router_gain)


def pair_steps(master_down, second_down, router_weight, router_gain):
    experts, inner, width = master_down.shape
    n = experts * inner
    m, s = in_hbm(master_down.reshape(n, width)), in_hbm(second_down.reshape(n, width))
    head = sum(HEAD) * LANES

    own0 = sums_of(m, s, 0, head)
    other0 = swap(own0)
    row, out, recvs = 0, None, []
    for i, size in enumerate((*HEAD, *cuts((n - head) // LANES))):
        late = row >= head
        send, out = norm_of(m, s, *((own1, other1, head) if late else (own0, other0, 0)), row, size * LANES, out)
        recvs.append((row, swap(send)))
        row += size * LANES
        if i == 0:
            own1 = sums_of(m, s, head, n - head, send)
            other1 = swap(own1)

    part_router = (router_weight * router_gain[:, None]).astype(jnp.bfloat16)
    me = lax.axis_index("zero")
    other_router = swap(part_router)
    low, high = jnp.where(me == 0, part_router, other_router), jnp.where(me == 0, other_router, part_router)
    serve_router = lax.all_gather(jnp.concatenate([low, high], 0), "bank", axis=1, tiled=True)

    for row, recv in recvs:
        out = place(recv, out, row)
    total = jnp.concatenate([own0 + other0, own1 + other1], 0)
    scale_down = jnp.sqrt(total).reshape(experts, inner)
    return out.reshape(experts, inner, 2 * width), scale_down, serve_router


def gather_body(master_down, second_down, router_weight, router_gain):
    merged_down = master_down + second_down.astype(jnp.float32)
    total_down = lax.psum(jnp.sum(merged_down * merged_down, axis=2), "zero")
    scale_down = jnp.sqrt(total_down)
    narrow_down = (merged_down / jnp.expand_dims(scale_down, 2)).astype(jnp.bfloat16)
    final_down = lax.all_gather(narrow_down, "zero", axis=2, tiled=True)
    part_router = (router_weight * router_gain[:, None]).astype(jnp.bfloat16)
    row_router = lax.all_gather(part_router, "zero", axis=0, tiled=True)
    serve_router = lax.all_gather(row_router, "bank", axis=1, tiled=True)
    return (final_down, scale_down, serve_router)


def solution(mesh):
    pair = mesh.shape["zero"] == 2
    return jax.shard_map(
        pair_body if pair else gather_body,
        mesh=mesh,
        in_specs=(P("bank", None, "zero"), P("bank", None, "zero"), P("zero", "bank"), P("zero")),
        out_specs=(P("bank", None, None), P("bank", None), P()),
        check_vma=False,
    )
```

```python
import functools

import jax
import jax.numpy as jnp
from jax import lax
from jax.experimental import pallas as pl
from jax.experimental.pallas import tpu as pltpu
from jax.sharding import PartitionSpec as P


LANES = 128
PAIR = ((0, 1), (1, 0))
ANY = pl.BlockSpec(memory_space=pl.ANY)
VMEM = pl.BlockSpec(memory_space=pltpu.VMEM)
EARLY = 32
GROUPS = ((1,), (2, 1), (8, 4))
LEAST = 24


def cost(us):
    return pl.CostEstimate(flops=int(us * 1e6), bytes_accessed=1024, transcendentals=0)


def params():
    return pltpu.CompilerParams(vmem_limit_bytes=16 * 1024 * 1024)


def lane_tiles(ref):
    return [pl.ds(k * LANES, LANES) for k in range(ref.shape[-1] // LANES)]


def block_rows(b):
    return pl.ds(b * LANES, LANES)


def merged_tile(m_ref, s_ref, rows, cols):
    return m_ref[rows, cols] + s_ref[rows, cols].astype(jnp.float32)


def row_scales(own, other):
    inverse = 1.0 / jnp.sqrt(own + other)
    return jnp.broadcast_to(inverse, (LANES, LANES)).T


def head_kernel(first, early, m_hbm, s_hbm, *refs):
    sums_ref, merged_ref = refs[:2]
    m_ref, s_ref, sems = refs[-3:]
    blocks = merged_ref.shape[0] // LANES
    copies = []
    for b in range(blocks):
        there = pl.ds(first + b * LANES, LANES)
        copies.append(pltpu.make_async_copy(m_hbm.at[there], m_ref.at[block_rows(b)], sems.at[2 * b]))
        copies.append(pltpu.make_async_copy(s_hbm.at[there], s_ref.at[block_rows(b)], sems.at[2 * b + 1]))
    for copy in copies:
        copy.start()
    for b in range(blocks):
        copies[2 * b].wait()
        copies[2 * b + 1].wait()
        acc = jnp.zeros((LANES, LANES), jnp.float32)
        for cols in lane_tiles(m_ref):
            v = merged_tile(m_ref, s_ref, block_rows(b), cols)
            merged_ref[block_rows(b), cols] = v
            if early and b == 0:
                refs[2][:, cols] = v[:early]
            acc = acc + v * v
        sums_ref[b] = jnp.sum(acc.T, axis=0, keepdims=True)


def head_norm_kernel(first, merged_ref, own_ref, other_ref, *refs):
    send_ref = refs[-1]
    count, row = send_ref.shape[0], first
    while row < first + count:
        b, skip = row // LANES, row % LANES
        rows = min(LANES - skip, first + count - row)
        inverse = row_scales(own_ref[b], other_ref[b])[skip : skip + rows]
        for cols in lane_tiles(merged_ref):
            v = merged_ref[pl.ds(row, rows), cols] * inverse
            send_ref[pl.ds(row - first, rows), cols] = v.astype(jnp.bfloat16)
        row += rows


def sums_kernel(m_ref, s_ref, *refs):
    sums_ref = refs[-1]
    for b in range(m_ref.shape[0] // LANES):
        acc = jnp.zeros((LANES, LANES), jnp.float32)
        for cols in lane_tiles(m_ref):
            v = merged_tile(m_ref, s_ref, block_rows(b), cols)
            acc = acc + v * v
        sums_ref[b] = jnp.sum(acc.T, axis=0, keepdims=True)


def norm_kernel(m_ref, s_ref, own_ref, other_ref, *refs):
    send_ref, out_ref = refs[-2:]
    for b in range(m_ref.shape[0] // LANES):
        inverse = row_scales(own_ref[b], other_ref[b])
        for cols in lane_tiles(m_ref):
            r = (merged_tile(m_ref, s_ref, block_rows(b), cols) * inverse).astype(jnp.bfloat16)
            send_ref[block_rows(b), cols] = r
            out_ref[block_rows(b), cols] = r


def received_half(out_ref, row, shape):
    rows, width = shape
    side = pl.multiple_of((1 - lax.axis_index("zero")) * width, LANES)
    return out_ref.at[pl.ds(row, rows), pl.ds(side, width)]


def place_kernel(row, recv_ref, _, out_ref, sem):
    copy = pltpu.make_async_copy(recv_ref, received_half(out_ref, row, recv_ref.shape), sem)
    copy.start()
    copy.wait()


def place_early_kernel(recv_ref, own_ref, other_ref, _, out_ref, held_ref, sem):
    rows = recv_ref.shape[0]
    inverse = row_scales(own_ref[0], other_ref[0])[:rows]
    for cols in lane_tiles(recv_ref):
        held_ref[:, cols] = (recv_ref[:, cols] * inverse).astype(jnp.bfloat16)
    copy = pltpu.make_async_copy(held_ref, received_half(out_ref, 0, recv_ref.shape), sem)
    copy.start()
    copy.wait()


def in_hbm(x):
    return pltpu.with_memory_space_constraint(x, pltpu.HBM)


def in_vmem(x):
    return pltpu.with_memory_space_constraint(x, pltpu.VMEM)


def whole_of(m):
    return jax.ShapeDtypeStruct((m.shape[0], 2 * m.shape[1]), jnp.bfloat16)


def sums_shape(blocks):
    return jax.ShapeDtypeStruct((blocks, 1, LANES), jnp.float32)


def head_of(m, s, first, blocks, early, after=()):
    rows, width = blocks * LANES, m.shape[1]
    shapes = [sums_shape(blocks), jax.ShapeDtypeStruct((rows, width), jnp.float32)]
    shapes += [jax.ShapeDtypeStruct((early, width), jnp.float32)] if early else []
    return pl.pallas_call(
        functools.partial(head_kernel, first, early) if not after else after_of(functools.partial(head_kernel, first, early), 2, len(after)),
        in_specs=[ANY, ANY] + [ANY] * len(after),
        out_specs=[VMEM] * len(shapes),
        out_shape=shapes,
        scratch_shapes=[
            pltpu.VMEM((rows, width), m.dtype),
            pltpu.VMEM((rows, width), s.dtype),
            pltpu.SemaphoreType.DMA((2 * blocks,)),
        ],
        compiler_params=params(),
        cost_estimate=cost(1),
        name="head",
    )(m, s, *after)


def after_of(kernel, at, count):
    def held(*refs):
        return kernel(*refs[:at], *refs[at + count :])

    return held


def head_norm_of(merged, own, other, first, count):
    return pl.pallas_call(
        functools.partial(head_norm_kernel, first),
        in_specs=[VMEM] * 3,
        out_specs=VMEM,
        out_shape=jax.ShapeDtypeStruct((count, merged.shape[1]), jnp.bfloat16),
        compiler_params=params(),
        cost_estimate=cost(1),
        name="head_norm",
    )(merged, own, other)


def step_rows(*counts):
    for rows in (512, 256):
        if all(count % rows == 0 for count in counts):
            return rows
    return LANES


def sums_of(m, s, first, count, after):
    rows, width = step_rows(first, count), m.shape[1]
    at = first // rows
    block = pl.BlockSpec((rows, width), lambda i: (at + i, 0))
    return pl.pallas_call(
        after_of(sums_kernel, 2, 1),
        grid=(count // rows,),
        in_specs=[block, block, ANY],
        out_specs=pl.BlockSpec((rows // LANES, 1, LANES), lambda i: (i, 0, 0)),
        out_shape=sums_shape(count // LANES),
        compiler_params=params(),
        cost_estimate=cost(count * 0.002),
        name="sums",
    )(m, s, after)


def norm_of(m, s, own, other, base, first, count, out):
    rows, width = step_rows(first, first - base, count), m.shape[1]
    at, near = first // rows, (first - base) // rows
    block = pl.BlockSpec((rows, width), lambda i: (at + i, 0))
    sums = pl.BlockSpec((rows // LANES, 1, LANES), lambda i: (near + i, 0, 0))
    held = [] if out is None else [out]
    return pl.pallas_call(
        norm_kernel,
        grid=(count // rows,),
        in_specs=[block, block, sums, sums] + [ANY] * len(held),
        out_specs=[
            pl.BlockSpec((rows, width), lambda i: (i, 0)),
            pl.BlockSpec((rows, width), lambda i: (at + i, lax.axis_index("zero"))),
        ],
        out_shape=[jax.ShapeDtypeStruct((count, width), jnp.bfloat16), whole_of(m)],
        input_output_aliases={4: 1} if held else {},
        compiler_params=params(),
        cost_estimate=cost(count * 0.003),
        name="norm",
    )(m, s, own, other, *held)


def place(recv, out, row):
    return pl.pallas_call(
        functools.partial(place_kernel, row),
        in_specs=[VMEM, ANY],
        out_specs=ANY,
        out_shape=jax.ShapeDtypeStruct(out.shape, out.dtype),
        scratch_shapes=[pltpu.SemaphoreType.DMA],
        input_output_aliases={1: 0},
        compiler_params=params(),
        cost_estimate=cost(1),
        name="place",
    )(recv, out)


def place_early(recv, own, other, out):
    return pl.pallas_call(
        place_early_kernel,
        in_specs=[VMEM, VMEM, VMEM, ANY],
        out_specs=ANY,
        out_shape=jax.ShapeDtypeStruct(out.shape, out.dtype),
        scratch_shapes=[pltpu.VMEM(recv.shape, jnp.bfloat16), pltpu.SemaphoreType.DMA],
        input_output_aliases={3: 0},
        compiler_params=params(),
        cost_estimate=cost(1),
        name="place_early",
    )(recv, own, other, out)


def swap(x):
    return lax.ppermute(x, "zero", PAIR)


def last_cuts(blocks):
    sizes = []
    while blocks > 12:
        sizes.append(8)
        blocks -= 8
    while blocks > 1:
        sizes.append(blocks // 2)
        blocks -= blocks // 2
    return (*sizes, 1)


def plan(blocks):
    return (*GROUPS, last_cuts(blocks - sum(map(sum, GROUPS))))


def pair_steps(master_down, second_down, router_weight, router_gain):
    experts, inner, width = master_down.shape
    n = experts * inner
    m, s = in_hbm(master_down.reshape(n, width)), in_hbm(second_down.reshape(n, width))
    groups = plan(n // LANES)

    own0, merged0, early = head_of(m, s, 0, 1, EARLY)
    sums = [(own0, swap(own0))]
    other_early = swap(early)
    own1, merged1 = head_of(m, s, LANES, sum(groups[1]), 0, (early,))
    sums.append((own1, swap(own1)))
    heads = (merged0, merged1)

    out, recvs, row, i = None, [], 0, 0
    for g, chunks in enumerate(groups):
        base = row
        for c, size in enumerate(chunks):
            count = size * LANES
            if g < 2:
                skip = EARLY if row == 0 else 0
                send = head_norm_of(heads[g], *sums[g], row - base + skip, count - skip)
            else:
                skip = 0
                send, out = norm_of(m, s, *sums[g], base, row, count, out)
            if row + count < n:
                recvs.append((row + skip, swap(send)))
            else:
                half = count // 2
                recvs.append((row, swap(send[:half])))
                recvs.append((row + half, swap(send[half:])))
            row += count
            if g + 1 == len(sums) and g + 1 < len(groups) and c + 1 == max(1, len(chunks) - 1):
                first, rest = base + sum(chunks) * LANES, sum(groups[g + 1]) * LANES
                own = sums_of(m, s, first, rest, send)
                sums.append((own, swap(own)))
            i += 1

    _, out = norm_of(m, s, *sums[0], 0, 0, LANES, out)
    _, out = norm_of(m, s, *sums[1], LANES, LANES, sum(groups[1]) * LANES, out)

    part_router = (router_weight * router_gain[:, None]).astype(jnp.bfloat16)
    me = lax.axis_index("zero")
    other_router = swap(part_router)
    low, high = jnp.where(me == 0, part_router, other_router), jnp.where(me == 0, other_router, part_router)
    serve_router = lax.all_gather(jnp.concatenate([low, high], 0), "bank", axis=1, tiled=True)

    out = place_early(other_early, *sums[0], out)
    for row, recv in recvs[:-1]:
        out = place(recv, out, row)
    row, recv = recvs[-1]
    out = place(in_vmem(recv), out, row)
    total = jnp.concatenate([own + other for own, other in sums], 0)
    scale_down = jnp.sqrt(total).reshape(experts, inner)
    return out.reshape(experts, inner, 2 * width), scale_down, serve_router


def gather_body(master_down, second_down, router_weight, router_gain):
    merged_down = master_down + second_down.astype(jnp.float32)
    total_down = lax.psum(jnp.sum(merged_down * merged_down, axis=2), "zero")
    scale_down = jnp.sqrt(total_down)
    narrow_down = (merged_down / jnp.expand_dims(scale_down, 2)).astype(jnp.bfloat16)
    final_down = lax.all_gather(narrow_down, "zero", axis=2, tiled=True)
    part_router = (router_weight * router_gain[:, None]).astype(jnp.bfloat16)
    row_router = lax.all_gather(part_router, "zero", axis=0, tiled=True)
    serve_router = lax.all_gather(row_router, "bank", axis=1, tiled=True)
    return (final_down, scale_down, serve_router)


def solution(mesh):
    specs = dict(
        mesh=mesh,
        in_specs=(P("bank", None, "zero"), P("bank", None, "zero"), P("zero", "bank"), P("zero")),
        out_specs=(P("bank", None, None), P("bank", None), P()),
        check_vma=False,
    )
    general = jax.shard_map(gather_body, **specs)

    def step(master_down, *rest):
        experts, inner, width = master_down.shape
        blocks, over = divmod(experts // mesh.shape["bank"] * inner, LANES)
        if mesh.shape["zero"] != 2 or over or blocks < LEAST or width % (2 * LANES):
            return general(master_down, *rest)
        return jax.shard_map(pair_steps, **specs)(master_down, *rest)

    return step
```

```python
import functools

import jax
import jax.numpy as jnp
from jax import lax
from jax.experimental import pallas as pl
from jax.experimental.pallas import tpu as pltpu
from jax.sharding import PartitionSpec as P


LANES = 128
PAIR = ((0, 1), (1, 0))
ANY = pl.BlockSpec(memory_space=pl.ANY)
VMEM = pl.BlockSpec(memory_space=pltpu.VMEM)
EARLY = 32
HEAD, NEXT = 2, 6
LONG = 8
LAST = (64, 32, 32)
LEAST = 24


def cost(us):
    return pl.CostEstimate(flops=int(us * 1e6), bytes_accessed=1024, transcendentals=0)


def params(mib):
    return pltpu.CompilerParams(vmem_limit_bytes=mib * 1024 * 1024)


def lane_tiles(ref):
    return [pl.ds(k * LANES, LANES) for k in range(ref.shape[-1] // LANES)]


def block_rows(b):
    return pl.ds(b * LANES, LANES)


def merged_tile(m_ref, s_ref, rows, cols):
    return m_ref[rows, cols] + s_ref[rows, cols].astype(jnp.float32)


def row_scales(own, other):
    inverse = 1.0 / jnp.sqrt(own + other)
    return jnp.broadcast_to(inverse, (LANES, LANES)).T


def head_kernel(first, early, m_hbm, s_hbm, *refs):
    sums_ref, merged_ref = refs[:2]
    m_ref, s_ref, sems = refs[-3:]
    blocks = merged_ref.shape[0] // LANES
    copies = []
    for b in range(blocks):
        there = pl.ds(first + b * LANES, LANES)
        copies.append(pltpu.make_async_copy(m_hbm.at[there], m_ref.at[block_rows(b)], sems.at[2 * b]))
        copies.append(pltpu.make_async_copy(s_hbm.at[there], s_ref.at[block_rows(b)], sems.at[2 * b + 1]))
    for copy in copies:
        copy.start()
    for b in range(blocks):
        copies[2 * b].wait()
        copies[2 * b + 1].wait()
        acc = jnp.zeros((LANES, LANES), jnp.float32)
        for cols in lane_tiles(m_ref):
            v = merged_tile(m_ref, s_ref, block_rows(b), cols)
            merged_ref[block_rows(b), cols] = v
            if early and b == 0:
                refs[2][:, cols] = v[:early]
            acc = acc + v * v
        sums_ref[b] = jnp.sum(acc.T, axis=0, keepdims=True)


def head_norm_kernel(cuts, merged_ref, own_ref, other_ref, *send_refs):
    for (first, count), send_ref in zip(cuts, send_refs, strict=True):
        row = first
        while row < first + count:
            b, skip = row // LANES, row % LANES
            rows = min(LANES - skip, first + count - row)
            inverse = row_scales(own_ref[b], other_ref[b])[skip : skip + rows]
            for cols in lane_tiles(merged_ref):
                v = merged_ref[pl.ds(row, rows), cols] * inverse
                send_ref[pl.ds(row - first, rows), cols] = v.astype(jnp.bfloat16)
            row += rows


def sums_kernel(m_ref, s_ref, *refs):
    sums_ref = refs[-1]
    for b in range(m_ref.shape[0] // LANES):
        acc = jnp.zeros((LANES, LANES), jnp.float32)
        for cols in lane_tiles(m_ref):
            v = merged_tile(m_ref, s_ref, block_rows(b), cols)
            acc = acc + v * v
        sums_ref[b] = jnp.sum(acc.T, axis=0, keepdims=True)


def norm_kernel(m_ref, s_ref, own_ref, other_ref, *refs):
    send_ref, out_ref = refs[-2:]
    for b in range(m_ref.shape[0] // LANES):
        inverse = row_scales(own_ref[b], other_ref[b])
        for cols in lane_tiles(m_ref):
            r = (merged_tile(m_ref, s_ref, block_rows(b), cols) * inverse).astype(jnp.bfloat16)
            send_ref[block_rows(b), cols] = r
            out_ref[block_rows(b), cols] = r


def received_half(out_ref, row, shape):
    rows, width = shape
    side = pl.multiple_of((1 - lax.axis_index("zero")) * width, LANES)
    return out_ref.at[pl.ds(row, rows), pl.ds(side, width)]


def place_kernel(row, recv_ref, _, out_ref, sem):
    copy = pltpu.make_async_copy(recv_ref, received_half(out_ref, row, recv_ref.shape), sem)
    copy.start()
    copy.wait()


def place_early_kernel(recv_ref, own_ref, other_ref, _, out_ref, held_ref, sem):
    rows = recv_ref.shape[0]
    inverse = row_scales(own_ref[0], other_ref[0])[:rows]
    for cols in lane_tiles(recv_ref):
        held_ref[:, cols] = (recv_ref[:, cols] * inverse).astype(jnp.bfloat16)
    copy = pltpu.make_async_copy(held_ref, received_half(out_ref, 0, recv_ref.shape), sem)
    copy.start()
    copy.wait()


def scale_kernel(inner, *refs):
    out_ref = refs[-1]
    block = 0
    for own_ref, other_ref in zip(refs[:-1:2], refs[1:-1:2], strict=True):
        for b in range(own_ref.shape[0]):
            expert, at = divmod(block * LANES, inner)
            out_ref[pl.ds(expert, 1), pl.ds(at, LANES)] = jnp.sqrt(own_ref[b] + other_ref[b])
            block += 1


def router_kernel(gathered_ref, out_ref):
    devices, columns, _ = gathered_ref.shape
    for d in range(devices):
        out_ref[pl.ds(d * columns, columns), :] = gathered_ref[d]


def in_hbm(x):
    return pltpu.with_memory_space_constraint(x, pltpu.HBM)


def whole_of(m):
    return jax.ShapeDtypeStruct((m.shape[0], 2 * m.shape[1]), jnp.bfloat16)


def sums_shape(blocks):
    return jax.ShapeDtypeStruct((blocks, 1, LANES), jnp.float32)


def head_of(m, s, first, blocks, early, after=()):
    rows, width = blocks * LANES, m.shape[1]
    shapes = [sums_shape(blocks), jax.ShapeDtypeStruct((rows, width), jnp.float32)]
    shapes += [jax.ShapeDtypeStruct((early, width), jnp.float32)] if early else []
    return pl.pallas_call(
        after_of(functools.partial(head_kernel, first, early), 2, len(after)),
        in_specs=[ANY, ANY] + [ANY] * len(after),
        out_specs=[VMEM] * len(shapes),
        out_shape=shapes,
        scratch_shapes=[
            pltpu.VMEM((rows, width), m.dtype),
            pltpu.VMEM((rows, width), s.dtype),
            pltpu.SemaphoreType.DMA((2 * blocks,)),
        ],
        compiler_params=params(12),
        cost_estimate=cost(1),
        name="head",
    )(m, s, *after)


def after_of(kernel, at, count):
    def held(*refs):
        return kernel(*refs[:at], *refs[at + count :])

    return held


def head_norm_of(merged, own, other, cuts):
    return pl.pallas_call(
        functools.partial(head_norm_kernel, cuts),
        in_specs=[VMEM] * 3,
        out_specs=[VMEM] * len(cuts),
        out_shape=[jax.ShapeDtypeStruct((count, merged.shape[1]), jnp.bfloat16) for _, count in cuts],
        compiler_params=params(8),
        cost_estimate=cost(1),
        name="head_norm",
    )(merged, own, other)


def scale_of(sums, experts, inner):
    refs = [x for pair in sums for x in pair]
    return pl.pallas_call(
        functools.partial(scale_kernel, inner),
        in_specs=[VMEM] * len(refs),
        out_specs=VMEM,
        out_shape=jax.ShapeDtypeStruct((experts, inner), jnp.float32),
        compiler_params=params(2),
        cost_estimate=cost(1),
        name="scale",
    )(*refs)


def router_of(gathered):
    devices, columns, rows = gathered.shape
    return pl.pallas_call(
        router_kernel,
        in_specs=[VMEM],
        out_specs=VMEM,
        out_shape=jax.ShapeDtypeStruct((devices * columns, rows), gathered.dtype),
        compiler_params=params(4),
        cost_estimate=cost(1),
        name="router",
    )(gathered)


def step_rows(*counts):
    for rows in (512, 256):
        if all(count % rows == 0 for count in counts):
            return rows
    return LANES


def sums_of(m, s, first, count, after):
    rows, width = step_rows(first, count), m.shape[1]
    at = first // rows
    block = pl.BlockSpec((rows, width), lambda i: (at + i, 0))
    return pl.pallas_call(
        after_of(sums_kernel, 2, 1),
        grid=(count // rows,),
        in_specs=[block, block, ANY],
        out_specs=pl.BlockSpec((rows // LANES, 1, LANES), lambda i: (i, 0, 0)),
        out_shape=sums_shape(count // LANES),
        compiler_params=params(12),
        cost_estimate=cost(count * 0.002),
        name="sums",
    )(m, s, after)


def norm_of(m, s, own, other, base, first, count, out):
    rows, width = step_rows(first, first - base, count), m.shape[1]
    at, near = first // rows, (first - base) // rows
    block = pl.BlockSpec((rows, width), lambda i: (at + i, 0))
    sums = pl.BlockSpec((rows // LANES, 1, LANES), lambda i: (near + i, 0, 0))
    held = [] if out is None else [out]
    return pl.pallas_call(
        norm_kernel,
        grid=(count // rows,),
        in_specs=[block, block, sums, sums] + [ANY] * len(held),
        out_specs=[
            pl.BlockSpec((rows, width), lambda i: (i, 0)),
            pl.BlockSpec((rows, width), lambda i: (at + i, lax.axis_index("zero"))),
        ],
        out_shape=[jax.ShapeDtypeStruct((count, width), jnp.bfloat16), whole_of(m)],
        input_output_aliases={4: 1} if held else {},
        compiler_params=params(14),
        cost_estimate=cost(count * 0.003),
        name="norm",
    )(m, s, own, other, *held)


def place(recv, out, row):
    return pl.pallas_call(
        functools.partial(place_kernel, row),
        in_specs=[VMEM, ANY],
        out_specs=ANY,
        out_shape=jax.ShapeDtypeStruct(out.shape, out.dtype),
        scratch_shapes=[pltpu.SemaphoreType.DMA],
        input_output_aliases={1: 0},
        compiler_params=params(6),
        cost_estimate=cost(1),
        name="place",
    )(recv, out)


def place_early(recv, own, other, out):
    return pl.pallas_call(
        place_early_kernel,
        in_specs=[VMEM, VMEM, VMEM, ANY],
        out_specs=ANY,
        out_shape=jax.ShapeDtypeStruct(out.shape, out.dtype),
        scratch_shapes=[pltpu.VMEM(recv.shape, jnp.bfloat16), pltpu.SemaphoreType.DMA],
        input_output_aliases={3: 0},
        compiler_params=params(2),
        cost_estimate=cost(1),
        name="place_early",
    )(recv, own, other, out)


def swap(x):
    return lax.ppermute(x, "zero", PAIR)


def long_cuts(blocks):
    sizes = []
    while blocks > LONG + 4:
        sizes.append(LONG)
        blocks -= LONG
    while blocks > 1:
        sizes.append((blocks + 1) // 2)
        blocks //= 2
    return sizes + [1] * blocks


def pair_steps(master_down, second_down, router_weight, router_gain):
    experts, inner, width = master_down.shape
    n = experts * inner
    m, s = in_hbm(master_down.reshape(n, width)), in_hbm(second_down.reshape(n, width))
    head, near = HEAD * LANES, (HEAD + NEXT) * LANES
    recvs = []

    own0, merged0, early = head_of(m, s, 0, HEAD, EARLY)
    sums0 = own0, swap(own0)
    other_early = swap(early)
    half = EARLY + (head - EARLY) // 32 * 16
    send_a, send_b = head_norm_of(merged0, *sums0, ((EARLY, half - EARLY), (half, head - half)))
    recvs.append((EARLY, swap(send_a)))
    own1, merged1 = head_of(m, s, head, NEXT, 0, (send_a,))
    sums1 = own1, swap(own1)
    recvs.append((half, swap(send_b)))

    half = NEXT // 2 * LANES
    (send_a,) = head_norm_of(merged1, *sums1, ((0, half),))
    recvs.append((head, swap(send_a)))
    own2 = sums_of(m, s, near, n - near, send_a)
    sums2 = own2, swap(own2)
    (send_b,) = head_norm_of(merged1, *sums1, ((half, NEXT * LANES - half),))
    recvs.append((head + half, swap(send_b)))
    part_router = (router_weight.T * router_gain).astype(jnp.bfloat16)
    other_router = swap(part_router)

    out, row, label = None, near, 4
    for size in long_cuts(n // LANES - HEAD - NEXT - 1):
        send, out = norm_of(m, s, *sums2, near, row, size * LANES, out)
        recvs.append((row, swap(send)))
        row += size * LANES
        label += 1
    cuts, at = [], 0
    for rows in LAST:
        cuts.append((at, rows))
        at += rows
    _, merged = head_of(m, s, n - LANES, 1, 0, (send,))
    sends = head_norm_of(merged, *(x[-1:] for x in sums2), tuple(cuts))
    for (at, _), send in zip(cuts, sends, strict=True):
        recvs.append((n - LANES + at, swap(send)))
        label += 1

    _, out = norm_of(m, s, *sums0, 0, 0, head, out)
    _, out = norm_of(m, s, *sums1, head, head, near - head, out)
    _, out = norm_of(m, s, *sums2, near, n - LANES, LANES, out)
    scale_down = scale_of((sums0, sums1, sums2), experts, inner)

    first = lax.axis_index("zero") == 0
    low, high = jnp.where(first, part_router, other_router), jnp.where(first, other_router, part_router)
    serve_router = router_of(lax.all_gather(jnp.concatenate([low, high], 1), "bank")).T

    out = place_early(other_early, *sums0, out)
    for row, recv in recvs:
        out = place(recv, out, row)
    return out.reshape(experts, inner, 2 * width), scale_down, serve_router


def gather_body(master_down, second_down, router_weight, router_gain):
    merged_down = master_down + second_down.astype(jnp.float32)
    total_down = lax.psum(jnp.sum(merged_down * merged_down, axis=2), "zero")
    scale_down = jnp.sqrt(total_down)
    narrow_down = (merged_down / jnp.expand_dims(scale_down, 2)).astype(jnp.bfloat16)
    final_down = lax.all_gather(narrow_down, "zero", axis=2, tiled=True)
    part_router = (router_weight * router_gain[:, None]).astype(jnp.bfloat16)
    row_router = lax.all_gather(part_router, "zero", axis=0, tiled=True)
    serve_router = lax.all_gather(row_router, "bank", axis=1, tiled=True)
    return (final_down, scale_down, serve_router)


def solution(mesh):
    specs = dict(
        mesh=mesh,
        in_specs=(P("bank", None, "zero"), P("bank", None, "zero"), P("zero", "bank"), P("zero")),
        out_specs=(P("bank", None, None), P("bank", None), P()),
        check_vma=False,
    )
    general = jax.shard_map(gather_body, **specs)

    def step(master_down, *rest):
        experts, inner, width = master_down.shape
        blocks, over = divmod(experts // mesh.shape["bank"] * inner, LANES)
        if mesh.shape["zero"] != 2 or over or blocks < LEAST or inner % LANES or width % LANES:
            return general(master_down, *rest)
        return jax.shard_map(pair_steps, **specs)(master_down, *rest)

    return step
```

```python
import functools

import jax
import jax.numpy as jnp
from jax import lax
from jax.experimental import pallas as pl
from jax.experimental.pallas import tpu as pltpu
from jax.sharding import PartitionSpec as P


LANES = 128
PAIR = ((0, 1), (1, 0))
ANY = pl.BlockSpec(memory_space=pl.ANY)
VMEM = pl.BlockSpec(memory_space=pltpu.VMEM)
EARLY = 48
HEAD, NEXT = 2, 6
LONG = 8
AHEAD = 12
LAST = (64, 32, 32)
LEAST = 24


def cost(us):
    return pl.CostEstimate(flops=int(us * 1e6), bytes_accessed=1024, transcendentals=0)


def params(mib):
    return pltpu.CompilerParams(vmem_limit_bytes=mib * 1024 * 1024)


def lane_tiles(ref):
    return [pl.ds(k * LANES, LANES) for k in range(ref.shape[-1] // LANES)]


def block_rows(b):
    return pl.ds(b * LANES, LANES)


def merged_tile(m_ref, s_ref, rows, cols):
    return m_ref[rows, cols] + s_ref[rows, cols].astype(jnp.float32)


def row_scales(own, other):
    inverse = 1.0 / jnp.sqrt(own + other)
    return jnp.broadcast_to(inverse, (LANES, LANES)).T


def head_kernel(first, early, m_hbm, s_hbm, *refs):
    sums_ref, merged_ref = refs[:2]
    m_ref, s_ref, sems = refs[-3:]
    blocks = merged_ref.shape[0] // LANES
    copies = []
    for b in range(blocks):
        there = pl.ds(first + b * LANES, LANES)
        copies.append(pltpu.make_async_copy(m_hbm.at[there], m_ref.at[block_rows(b)], sems.at[2 * b]))
        copies.append(pltpu.make_async_copy(s_hbm.at[there], s_ref.at[block_rows(b)], sems.at[2 * b + 1]))
    for copy in copies:
        copy.start()
    for b in range(blocks):
        copies[2 * b].wait()
        copies[2 * b + 1].wait()
        acc = jnp.zeros((LANES, LANES), jnp.float32)
        for cols in lane_tiles(m_ref):
            v = merged_tile(m_ref, s_ref, block_rows(b), cols)
            merged_ref[block_rows(b), cols] = v
            if early and b == 0:
                refs[2][:, cols] = v[:early]
            acc = acc + v * v
        sums_ref[b] = jnp.sum(acc.T, axis=0, keepdims=True)


def head_norm_kernel(cuts, merged_ref, own_ref, other_ref, *send_refs):
    for (first, count), send_ref in zip(cuts, send_refs, strict=True):
        row = first
        while row < first + count:
            b, skip = row // LANES, row % LANES
            rows = min(LANES - skip, first + count - row)
            inverse = row_scales(own_ref[b], other_ref[b])[skip : skip + rows]
            for cols in lane_tiles(merged_ref):
                v = merged_ref[pl.ds(row, rows), cols] * inverse
                send_ref[pl.ds(row - first, rows), cols] = v.astype(jnp.bfloat16)
            row += rows


def sums_kernel(m_ref, s_ref, *refs):
    sums_ref = refs[-1]
    for b in range(m_ref.shape[0] // LANES):
        acc = jnp.zeros((LANES, LANES), jnp.float32)
        for cols in lane_tiles(m_ref):
            v = merged_tile(m_ref, s_ref, block_rows(b), cols)
            acc = acc + v * v
        sums_ref[b] = jnp.sum(acc.T, axis=0, keepdims=True)


def norm_kernel(m_ref, s_ref, own_ref, other_ref, *refs):
    send_ref, out_ref = refs[-2:]
    for b in range(m_ref.shape[0] // LANES):
        inverse = row_scales(own_ref[b], other_ref[b])
        for cols in lane_tiles(m_ref):
            r = (merged_tile(m_ref, s_ref, block_rows(b), cols) * inverse).astype(jnp.bfloat16)
            send_ref[block_rows(b), cols] = r
            out_ref[block_rows(b), cols] = r


def received_half(out_ref, row, shape):
    rows, width = shape
    side = pl.multiple_of((1 - lax.axis_index("zero")) * width, LANES)
    return out_ref.at[pl.ds(row, rows), pl.ds(side, width)]


def place_kernel(row, recv_ref, _, out_ref, sem):
    copy = pltpu.make_async_copy(recv_ref, received_half(out_ref, row, recv_ref.shape), sem)
    copy.start()
    copy.wait()


def place_early_kernel(recv_ref, own_ref, other_ref, _, out_ref, held_ref, sem):
    rows = recv_ref.shape[0]
    inverse = row_scales(own_ref[0], other_ref[0])[:rows]
    for cols in lane_tiles(recv_ref):
        held_ref[:, cols] = (recv_ref[:, cols] * inverse).astype(jnp.bfloat16)
    copy = pltpu.make_async_copy(held_ref, received_half(out_ref, 0, recv_ref.shape), sem)
    copy.start()
    copy.wait()


def scale_kernel(inner, *refs):
    out_ref = refs[-1]
    block = 0
    for own_ref, other_ref in zip(refs[:-1:2], refs[1:-1:2], strict=True):
        for b in range(own_ref.shape[0]):
            expert, at = divmod(block * LANES, inner)
            out_ref[pl.ds(expert, 1), pl.ds(at, LANES)] = jnp.sqrt(own_ref[b] + other_ref[b])
            block += 1


def router_rows_kernel(own_ref, other_ref, out_ref):
    width = own_ref.shape[1]
    me = lax.axis_index("zero")
    for ref, at in ((own_ref, me), (other_ref, 1 - me)):
        out_ref[:, pl.ds(pl.multiple_of(at * width, LANES), width)] = ref[...]


def router_kernel(gathered_ref, out_ref):
    devices, columns, _ = gathered_ref.shape
    for d in range(devices):
        out_ref[pl.ds(d * columns, columns), :] = gathered_ref[d]


def in_hbm(x):
    return pltpu.with_memory_space_constraint(x, pltpu.HBM)


def whole_of(m):
    return jax.ShapeDtypeStruct((m.shape[0], 2 * m.shape[1]), jnp.bfloat16)


def sums_shape(blocks):
    return jax.ShapeDtypeStruct((blocks, 1, LANES), jnp.float32)


def head_of(m, s, first, blocks, early, after=()):
    rows, width = blocks * LANES, m.shape[1]
    shapes = [sums_shape(blocks), jax.ShapeDtypeStruct((rows, width), jnp.float32)]
    shapes += [jax.ShapeDtypeStruct((early, width), jnp.float32)] if early else []
    return pl.pallas_call(
        after_of(functools.partial(head_kernel, first, early), 2, len(after)),
        in_specs=[ANY, ANY] + [ANY] * len(after),
        out_specs=[VMEM] * len(shapes),
        out_shape=shapes,
        scratch_shapes=[
            pltpu.VMEM((rows, width), m.dtype),
            pltpu.VMEM((rows, width), s.dtype),
            pltpu.SemaphoreType.DMA((2 * blocks,)),
        ],
        compiler_params=params(12),
        cost_estimate=cost(1),
        name="head",
    )(m, s, *after)


def after_of(kernel, at, count):
    def held(*refs):
        return kernel(*refs[:at], *refs[at + count :])

    return held


def head_norm_of(merged, own, other, cuts):
    return pl.pallas_call(
        functools.partial(head_norm_kernel, cuts),
        in_specs=[VMEM] * 3,
        out_specs=[VMEM] * len(cuts),
        out_shape=[jax.ShapeDtypeStruct((count, merged.shape[1]), jnp.bfloat16) for _, count in cuts],
        compiler_params=params(8),
        cost_estimate=cost(1),
        name="head_norm",
    )(merged, own, other)


def scale_of(sums, experts, inner):
    refs = [x for pair in sums for x in pair]
    return pl.pallas_call(
        functools.partial(scale_kernel, inner),
        in_specs=[VMEM] * len(refs),
        out_specs=VMEM,
        out_shape=jax.ShapeDtypeStruct((experts, inner), jnp.float32),
        compiler_params=params(2),
        cost_estimate=cost(1),
        name="scale",
    )(*refs)


def router_rows_of(own, other):
    return pl.pallas_call(
        router_rows_kernel,
        in_specs=[VMEM] * 2,
        out_specs=VMEM,
        out_shape=jax.ShapeDtypeStruct((own.shape[0], 2 * own.shape[1]), own.dtype),
        compiler_params=params(2),
        cost_estimate=cost(1),
        name="router_rows",
    )(own, other)


def router_of(gathered):
    devices, columns, rows = gathered.shape
    return pl.pallas_call(
        router_kernel,
        in_specs=[VMEM],
        out_specs=VMEM,
        out_shape=jax.ShapeDtypeStruct((devices * columns, rows), gathered.dtype),
        compiler_params=params(4),
        cost_estimate=cost(1),
        name="router",
    )(gathered)


def step_rows(*counts):
    for rows in (512, 256):
        if all(count % rows == 0 for count in counts):
            return rows
    return LANES


def sums_of(m, s, first, count, after):
    rows, width = step_rows(first, count), m.shape[1]
    at = first // rows
    block = pl.BlockSpec((rows, width), lambda i: (at + i, 0))
    return pl.pallas_call(
        after_of(sums_kernel, 2, 1),
        grid=(count // rows,),
        in_specs=[block, block, ANY],
        out_specs=pl.BlockSpec((rows // LANES, 1, LANES), lambda i: (i, 0, 0)),
        out_shape=sums_shape(count // LANES),
        compiler_params=params(12),
        cost_estimate=cost(count * 0.002),
        name="sums",
    )(m, s, after)


def norm_of(m, s, own, other, base, first, count, out):
    rows, width = step_rows(first, first - base, count), m.shape[1]
    at, near = first // rows, (first - base) // rows
    block = pl.BlockSpec((rows, width), lambda i: (at + i, 0))
    sums = pl.BlockSpec((rows // LANES, 1, LANES), lambda i: (near + i, 0, 0))
    held = [] if out is None else [out]
    return pl.pallas_call(
        norm_kernel,
        grid=(count // rows,),
        in_specs=[block, block, sums, sums] + [ANY] * len(held),
        out_specs=[
            pl.BlockSpec((rows, width), lambda i: (i, 0)),
            pl.BlockSpec((rows, width), lambda i: (at + i, lax.axis_index("zero"))),
        ],
        out_shape=[jax.ShapeDtypeStruct((count, width), jnp.bfloat16), whole_of(m)],
        input_output_aliases={4: 1} if held else {},
        compiler_params=params(14),
        cost_estimate=cost(count * 0.003),
        name="norm",
    )(m, s, own, other, *held)


def place(recv, out, row):
    return pl.pallas_call(
        functools.partial(place_kernel, row),
        in_specs=[VMEM, ANY],
        out_specs=ANY,
        out_shape=jax.ShapeDtypeStruct(out.shape, out.dtype),
        scratch_shapes=[pltpu.SemaphoreType.DMA],
        input_output_aliases={1: 0},
        compiler_params=params(6),
        cost_estimate=cost(1),
        name="place",
    )(recv, out)


def place_early(recv, own, other, out):
    return pl.pallas_call(
        place_early_kernel,
        in_specs=[VMEM, VMEM, VMEM, ANY],
        out_specs=ANY,
        out_shape=jax.ShapeDtypeStruct(out.shape, out.dtype),
        scratch_shapes=[pltpu.VMEM(recv.shape, jnp.bfloat16), pltpu.SemaphoreType.DMA],
        input_output_aliases={3: 0},
        compiler_params=params(2),
        cost_estimate=cost(1),
        name="place_early",
    )(recv, own, other, out)


def swap(x):
    return lax.ppermute(x, "zero", PAIR)


def long_cuts(blocks):
    sizes = []
    while blocks > LONG + 4:
        sizes.append(LONG)
        blocks -= LONG
    while blocks > 1:
        sizes.append((blocks + 1) // 2)
        blocks //= 2
    return sizes + [1] * blocks


def pair_steps(master_down, second_down, router_weight, router_gain):
    experts, inner, width = master_down.shape
    n = experts * inner
    m, s = in_hbm(master_down.reshape(n, width)), in_hbm(second_down.reshape(n, width))
    head, near = HEAD * LANES, (HEAD + NEXT) * LANES
    recvs = []

    own0, merged0, early = head_of(m, s, 0, HEAD, EARLY)
    sums0 = own0, swap(own0)
    other_early = swap(early)
    half = EARLY + (head - EARLY) // 32 * 16
    send_a, send_b = head_norm_of(merged0, *sums0, ((EARLY, half - EARLY), (half, head - half)))
    recvs.append((EARLY, swap(send_a)))
    own1, merged1 = head_of(m, s, head, NEXT, 0, (send_a,))
    sums1 = own1, swap(own1)
    recvs.append((half, swap(send_b)))

    half = NEXT // 2 * LANES
    (send_a,) = head_norm_of(merged1, *sums1, ((0, half),))
    recvs.append((head, swap(send_a)))
    own2 = sums_of(m, s, near, n - near, send_a)
    sums2 = own2, swap(own2)
    (send_b,) = head_norm_of(merged1, *sums1, ((half, NEXT * LANES - half),))
    recvs.append((head + half, swap(send_b)))
    part_router = (router_weight.T * router_gain).astype(jnp.bfloat16)
    other_router = swap(part_router)

    rows = router_rows_of(part_router, other_router)
    serve_router = router_of(lax.all_gather(rows, "bank")).T

    def ready(out, ahead):
        if recvs[0][0] == EARLY:
            _, out = norm_of(m, s, *sums0, 0, 0, head, out)
            _, out = norm_of(m, s, *sums1, head, head, near - head, out)
            out = place_early(other_early, *sums0, out)
        while recvs and sum(recv.shape[0] for _, recv in recvs[1:]) >= ahead:
            at, recv = recvs.pop(0)
            out = place(recv, out, at)
        return out

    out, row, label = None, near, 4
    for size in long_cuts(n // LANES - HEAD - NEXT - 1):
        if label > 5:
            out = ready(out, AHEAD * LANES)
        send, out = norm_of(m, s, *sums2, near, row, size * LANES, out)
        recvs.append((row, swap(send)))
        row += size * LANES
        label += 1
    cuts, at = [], 0
    for rows in LAST:
        cuts.append((at, rows))
        at += rows
    _, merged = head_of(m, s, n - LANES, 1, 0, (send,))
    sends = head_norm_of(merged, *(x[-1:] for x in sums2), tuple(cuts))
    for (at, _), send in zip(cuts, sends, strict=True):
        recvs.append((n - LANES + at, swap(send)))
        label += 1
    _, out = norm_of(m, s, *sums2, near, n - LANES, LANES, out)
    scale_down = scale_of((sums0, sums1, sums2), experts, inner)
    out = ready(out, 0)
    return out.reshape(experts, inner, 2 * width), scale_down, serve_router


def gather_body(master_down, second_down, router_weight, router_gain):
    merged_down = master_down + second_down.astype(jnp.float32)
    total_down = lax.psum(jnp.sum(merged_down * merged_down, axis=2), "zero")
    scale_down = jnp.sqrt(total_down)
    narrow_down = (merged_down / jnp.expand_dims(scale_down, 2)).astype(jnp.bfloat16)
    final_down = lax.all_gather(narrow_down, "zero", axis=2, tiled=True)
    part_router = (router_weight * router_gain[:, None]).astype(jnp.bfloat16)
    row_router = lax.all_gather(part_router, "zero", axis=0, tiled=True)
    serve_router = lax.all_gather(row_router, "bank", axis=1, tiled=True)
    return (final_down, scale_down, serve_router)


def solution(mesh):
    specs = dict(
        mesh=mesh,
        in_specs=(P("bank", None, "zero"), P("bank", None, "zero"), P("zero", "bank"), P("zero")),
        out_specs=(P("bank", None, None), P("bank", None), P()),
        check_vma=False,
    )
    general = jax.shard_map(gather_body, **specs)

    def step(master_down, *rest):
        experts, inner, width = master_down.shape
        blocks, over = divmod(experts // mesh.shape["bank"] * inner, LANES)
        if mesh.shape["zero"] != 2 or over or blocks < LEAST or inner % LANES or width % LANES:
            return general(master_down, *rest)
        return jax.shard_map(pair_steps, **specs)(master_down, *rest)

    return step
```

```python
import functools

import jax
import jax.numpy as jnp
from jax import lax
from jax.experimental import pallas as pl
from jax.experimental.pallas import tpu as pltpu
from jax.sharding import PartitionSpec as P


LANES = 128
PAIR = ((0, 1), (1, 0))
ANY = pl.BlockSpec(memory_space=pl.ANY)
VMEM = pl.BlockSpec(memory_space=pltpu.VMEM)
EARLY = 80
HEAD, NEXT = 3, 5
LONG = 8
AHEAD = 12
LAST = (64, 32, 32)
LEAST = 40


def cost(us):
    return pl.CostEstimate(flops=int(us * 1e6), bytes_accessed=1024, transcendentals=0)


def params(mib):
    return pltpu.CompilerParams(vmem_limit_bytes=mib * 1024 * 1024)


def lane_tiles(ref):
    return [pl.ds(k * LANES, LANES) for k in range(ref.shape[-1] // LANES)]


def block_rows(b):
    return pl.ds(b * LANES, LANES)


def merged_tile(m_ref, s_ref, rows, cols):
    return m_ref[rows, cols] + s_ref[rows, cols].astype(jnp.float32)


def row_scales(own, other):
    inverse = 1.0 / jnp.sqrt(own + other)
    return jnp.broadcast_to(inverse, (LANES, LANES)).T


def head_kernel(first, early, m_hbm, s_hbm, *refs):
    sums_ref, merged_ref = refs[:2]
    m_ref, s_ref, sems = refs[-3:]
    blocks = merged_ref.shape[0] // LANES
    copies = []
    for b in range(blocks):
        there = pl.ds(first + b * LANES, LANES)
        copies.append(pltpu.make_async_copy(m_hbm.at[there], m_ref.at[block_rows(b)], sems.at[2 * b]))
        copies.append(pltpu.make_async_copy(s_hbm.at[there], s_ref.at[block_rows(b)], sems.at[2 * b + 1]))
    for copy in copies:
        copy.start()
    for b in range(blocks):
        copies[2 * b].wait()
        copies[2 * b + 1].wait()
        acc = jnp.zeros((LANES, LANES), jnp.float32)
        for cols in lane_tiles(m_ref):
            v = merged_tile(m_ref, s_ref, block_rows(b), cols)
            merged_ref[block_rows(b), cols] = v
            if early and b == 0:
                refs[2][:, cols] = v[:early].astype(jnp.bfloat16)
            acc = acc + v * v
        sums_ref[b] = jnp.sum(acc.T, axis=0, keepdims=True)


def head_norm_kernel(cuts, merged_ref, own_ref, other_ref, *send_refs):
    for (first, count), send_ref in zip(cuts, send_refs, strict=True):
        row = first
        while row < first + count:
            b, skip = row // LANES, row % LANES
            rows = min(LANES - skip, first + count - row)
            inverse = row_scales(own_ref[b], other_ref[b])[skip : skip + rows]
            for cols in lane_tiles(merged_ref):
                v = merged_ref[pl.ds(row, rows), cols] * inverse
                send_ref[pl.ds(row - first, rows), cols] = v.astype(jnp.bfloat16)
            row += rows


def sums_kernel(m_ref, s_ref, *refs):
    sums_ref = refs[-1]
    for b in range(m_ref.shape[0] // LANES):
        acc = jnp.zeros((LANES, LANES), jnp.float32)
        for cols in lane_tiles(m_ref):
            v = merged_tile(m_ref, s_ref, block_rows(b), cols)
            acc = acc + v * v
        sums_ref[b] = jnp.sum(acc.T, axis=0, keepdims=True)


def norm_kernel(m_ref, s_ref, own_ref, other_ref, *refs):
    send_ref, out_ref = refs[-2:]
    for b in range(m_ref.shape[0] // LANES):
        inverse = row_scales(own_ref[b], other_ref[b])
        for cols in lane_tiles(m_ref):
            r = (merged_tile(m_ref, s_ref, block_rows(b), cols) * inverse).astype(jnp.bfloat16)
            send_ref[block_rows(b), cols] = r
            out_ref[block_rows(b), cols] = r


def received_half(out_ref, row, shape):
    rows, width = shape
    side = pl.multiple_of((1 - lax.axis_index("zero")) * width, LANES)
    return out_ref.at[pl.ds(row, rows), pl.ds(side, width)]


def place_kernel(row, recv_ref, _, out_ref, sem):
    copy = pltpu.make_async_copy(recv_ref, received_half(out_ref, row, recv_ref.shape), sem)
    copy.start()
    copy.wait()


def place_early_kernel(recv_ref, own_ref, other_ref, _, out_ref, held_ref, sem):
    rows = recv_ref.shape[0]
    inverse = row_scales(own_ref[0], other_ref[0])[:rows]
    for cols in lane_tiles(recv_ref):
        held_ref[:, cols] = (recv_ref[:, cols].astype(jnp.float32) * inverse).astype(jnp.bfloat16)
    copy = pltpu.make_async_copy(held_ref, received_half(out_ref, 0, recv_ref.shape), sem)
    copy.start()
    copy.wait()


def scale_kernel(inner, *refs):
    out_ref = refs[-1]
    block = 0
    for own_ref, other_ref in zip(refs[:-1:2], refs[1:-1:2], strict=True):
        for b in range(own_ref.shape[0]):
            expert, at = divmod(block * LANES, inner)
            out_ref[pl.ds(expert, 1), pl.ds(at, LANES)] = jnp.sqrt(own_ref[b] + other_ref[b])
            block += 1


def router_rows_kernel(own_ref, other_ref, out_ref):
    width = own_ref.shape[1]
    me = lax.axis_index("zero")
    for ref, at in ((own_ref, me), (other_ref, 1 - me)):
        out_ref[:, pl.ds(pl.multiple_of(at * width, LANES), width)] = ref[...]


def router_kernel(gathered_ref, out_ref):
    devices, columns, _ = gathered_ref.shape
    for d in range(devices):
        out_ref[pl.ds(d * columns, columns), :] = gathered_ref[d]


def in_hbm(x):
    return pltpu.with_memory_space_constraint(x, pltpu.HBM)


def whole_of(m):
    return jax.ShapeDtypeStruct((m.shape[0], 2 * m.shape[1]), jnp.bfloat16)


def sums_shape(blocks):
    return jax.ShapeDtypeStruct((blocks, 1, LANES), jnp.float32)


def head_of(m, s, first, blocks, early, after=()):
    rows, width = blocks * LANES, m.shape[1]
    shapes = [sums_shape(blocks), jax.ShapeDtypeStruct((rows, width), jnp.float32)]
    shapes += [jax.ShapeDtypeStruct((early, width), jnp.bfloat16)] if early else []
    return pl.pallas_call(
        after_of(functools.partial(head_kernel, first, early), 2, len(after)),
        in_specs=[ANY, ANY] + [ANY] * len(after),
        out_specs=[VMEM] * len(shapes),
        out_shape=shapes,
        scratch_shapes=[
            pltpu.VMEM((rows, width), m.dtype),
            pltpu.VMEM((rows, width), s.dtype),
            pltpu.SemaphoreType.DMA((2 * blocks,)),
        ],
        compiler_params=params(12),
        cost_estimate=cost(1),
        name="head",
    )(m, s, *after)


def after_of(kernel, at, count):
    def held(*refs):
        return kernel(*refs[:at], *refs[at + count :])

    return held


def head_norm_of(merged, own, other, cuts):
    return pl.pallas_call(
        functools.partial(head_norm_kernel, cuts),
        in_specs=[VMEM] * 3,
        out_specs=[VMEM] * len(cuts),
        out_shape=[jax.ShapeDtypeStruct((count, merged.shape[1]), jnp.bfloat16) for _, count in cuts],
        compiler_params=params(8),
        cost_estimate=cost(1),
        name="head_norm",
    )(merged, own, other)


def scale_of(sums, experts, inner):
    refs = [x for pair in sums for x in pair]
    return pl.pallas_call(
        functools.partial(scale_kernel, inner),
        in_specs=[VMEM] * len(refs),
        out_specs=VMEM,
        out_shape=jax.ShapeDtypeStruct((experts, inner), jnp.float32),
        compiler_params=params(2),
        cost_estimate=cost(1),
        name="scale",
    )(*refs)


def router_rows_of(own, other):
    return pl.pallas_call(
        router_rows_kernel,
        in_specs=[VMEM] * 2,
        out_specs=VMEM,
        out_shape=jax.ShapeDtypeStruct((own.shape[0], 2 * own.shape[1]), own.dtype),
        compiler_params=params(2),
        cost_estimate=cost(1),
        name="router_rows",
    )(own, other)


def router_of(gathered):
    devices, columns, rows = gathered.shape
    return pl.pallas_call(
        router_kernel,
        in_specs=[VMEM],
        out_specs=VMEM,
        out_shape=jax.ShapeDtypeStruct((devices * columns, rows), gathered.dtype),
        compiler_params=params(4),
        cost_estimate=cost(1),
        name="router",
    )(gathered)


def step_rows(*counts):
    for rows in (512, 256):
        if all(count % rows == 0 for count in counts):
            return rows
    return LANES


def sums_of(m, s, first, count, after):
    rows, width = step_rows(first, count), m.shape[1]
    at = first // rows
    block = pl.BlockSpec((rows, width), lambda i: (at + i, 0))
    return pl.pallas_call(
        after_of(sums_kernel, 2, 1),
        grid=(count // rows,),
        in_specs=[block, block, ANY],
        out_specs=pl.BlockSpec((rows // LANES, 1, LANES), lambda i: (i, 0, 0)),
        out_shape=sums_shape(count // LANES),
        compiler_params=params(12),
        cost_estimate=cost(count * 0.002),
        name="sums",
    )(m, s, after)


def norm_of(m, s, own, other, base, first, count, out):
    rows, width = step_rows(first, first - base, count), m.shape[1]
    at, near = first // rows, (first - base) // rows
    block = pl.BlockSpec((rows, width), lambda i: (at + i, 0))
    sums = pl.BlockSpec((rows // LANES, 1, LANES), lambda i: (near + i, 0, 0))
    held = [] if out is None else [out]
    return pl.pallas_call(
        norm_kernel,
        grid=(count // rows,),
        in_specs=[block, block, sums, sums] + [ANY] * len(held),
        out_specs=[
            pl.BlockSpec((rows, width), lambda i: (i, 0)),
            pl.BlockSpec((rows, width), lambda i: (at + i, lax.axis_index("zero"))),
        ],
        out_shape=[jax.ShapeDtypeStruct((count, width), jnp.bfloat16), whole_of(m)],
        input_output_aliases={4: 1} if held else {},
        compiler_params=params(14),
        cost_estimate=cost(count * 0.003),
        name="norm",
    )(m, s, own, other, *held)


def place(recv, out, row):
    return pl.pallas_call(
        functools.partial(place_kernel, row),
        in_specs=[VMEM, ANY],
        out_specs=ANY,
        out_shape=jax.ShapeDtypeStruct(out.shape, out.dtype),
        scratch_shapes=[pltpu.SemaphoreType.DMA],
        input_output_aliases={1: 0},
        compiler_params=params(6),
        cost_estimate=cost(1),
        name="place",
    )(recv, out)


def place_early(recv, own, other, out):
    return pl.pallas_call(
        place_early_kernel,
        in_specs=[VMEM, VMEM, VMEM, ANY],
        out_specs=ANY,
        out_shape=jax.ShapeDtypeStruct(out.shape, out.dtype),
        scratch_shapes=[pltpu.VMEM(recv.shape, jnp.bfloat16), pltpu.SemaphoreType.DMA],
        input_output_aliases={3: 0},
        compiler_params=params(2),
        cost_estimate=cost(1),
        name="place_early",
    )(recv, own, other, out)


def swap(x):
    return lax.ppermute(x, "zero", PAIR)


def long_cuts(blocks):
    sizes = []
    while blocks > LONG + 4:
        sizes.append(LONG)
        blocks -= LONG
    while blocks > 1:
        sizes.append((blocks + 1) // 2)
        blocks //= 2
    return sizes + [1] * blocks


def pair_steps(master_down, second_down, router_weight, router_gain):
    experts, inner, width = master_down.shape
    n = experts * inner
    m, s = in_hbm(master_down.reshape(n, width)), in_hbm(second_down.reshape(n, width))
    head, near = HEAD * LANES, (HEAD + NEXT) * LANES
    recvs = []

    own0, merged0, early = head_of(m, s, 0, HEAD, EARLY)
    sums0 = own0, swap(own0)
    other_early = swap(early)
    half = EARLY + (head - EARLY) // 32 * 16
    send_a, send_b = head_norm_of(merged0, *sums0, ((EARLY, half - EARLY), (half, head - half)))
    recvs.append((EARLY, swap(send_a)))
    own1, merged1 = head_of(m, s, head, NEXT, 0, (send_a,))
    sums1 = own1, swap(own1)
    recvs.append((half, swap(send_b)))

    half = (NEXT + 1) // 2 * LANES
    (send_a,) = head_norm_of(merged1, *sums1, ((0, half),))
    recvs.append((head, swap(send_a)))
    own2 = sums_of(m, s, near, n - near, send_a)
    sums2 = own2, swap(own2)
    (send_b,) = head_norm_of(merged1, *sums1, ((half, NEXT * LANES - half),))
    recvs.append((head + half, swap(send_b)))
    part_router = (router_weight.T * router_gain).astype(jnp.bfloat16)
    other_router = swap(part_router)

    rows = router_rows_of(part_router, other_router)
    serve_router = router_of(lax.all_gather(rows, "bank")).T

    def ready(out, ahead):
        if recvs[0][0] == EARLY:
            _, out = norm_of(m, s, *sums0, 0, 0, head, out)
            _, out = norm_of(m, s, *sums1, head, head, near - head, out)
            out = place_early(other_early, *sums0, out)
        while recvs and sum(recv.shape[0] for _, recv in recvs[1:]) >= ahead:
            at, recv = recvs.pop(0)
            out = place(recv, out, at)
        return out

    out, row, label = None, near, 4
    for size in long_cuts(n // LANES - HEAD - NEXT - 1):
        if label > 5:
            out = ready(out, AHEAD * LANES)
        send, out = norm_of(m, s, *sums2, near, row, size * LANES, out)
        recvs.append((row, swap(send)))
        row += size * LANES
        label += 1
    cuts, at = [], 0
    for rows in LAST:
        cuts.append((at, rows))
        at += rows
    _, merged = head_of(m, s, n - LANES, 1, 0, (send,))
    sends = head_norm_of(merged, *(x[-1:] for x in sums2), tuple(cuts))
    for (at, _), send in zip(cuts, sends, strict=True):
        recvs.append((n - LANES + at, swap(send)))
        label += 1
    _, out = norm_of(m, s, *sums2, near, n - LANES, LANES, out)
    scale_down = scale_of((sums0, sums1, sums2), experts, inner)
    out = ready(out, 0)
    return out.reshape(experts, inner, 2 * width), scale_down, serve_router


def gather_body(master_down, second_down, router_weight, router_gain):
    merged_down = master_down + second_down.astype(jnp.float32)
    total_down = lax.psum(jnp.sum(merged_down * merged_down, axis=2), "zero")
    scale_down = jnp.sqrt(total_down)
    narrow_down = (merged_down / jnp.expand_dims(scale_down, 2)).astype(jnp.bfloat16)
    final_down = lax.all_gather(narrow_down, "zero", axis=2, tiled=True)
    part_router = (router_weight * router_gain[:, None]).astype(jnp.bfloat16)
    row_router = lax.all_gather(part_router, "zero", axis=0, tiled=True)
    serve_router = lax.all_gather(row_router, "bank", axis=1, tiled=True)
    return (final_down, scale_down, serve_router)


def solution(mesh):
    specs = dict(
        mesh=mesh,
        in_specs=(P("bank", None, "zero"), P("bank", None, "zero"), P("zero", "bank"), P("zero")),
        out_specs=(P("bank", None, None), P("bank", None), P()),
        check_vma=False,
    )
    general = jax.shard_map(gather_body, **specs)

    def step(master_down, *rest):
        experts, inner, width = master_down.shape
        blocks, over = divmod(experts // mesh.shape["bank"] * inner, LANES)
        if mesh.shape["zero"] != 2 or over or blocks < LEAST or inner % LANES or width % LANES:
            return general(master_down, *rest)
        return jax.shard_map(pair_steps, **specs)(master_down, *rest)

    return step
```

```python
import functools

import jax
import jax.numpy as jnp
from jax import lax
from jax.experimental import pallas as pl
from jax.experimental.pallas import tpu as pltpu
from jax.sharding import PartitionSpec as P


LANES = 128
PAIR = ((0, 1), (1, 0))
ANY = pl.BlockSpec(memory_space=pl.ANY)
VMEM = pl.BlockSpec(memory_space=pltpu.VMEM)
PARTS = (40, 48)
EARLY = sum(PARTS)
HEAD, NEXT = 2, 6
LONG = 8
AHEAD = 12
LAST = (64, 32, 32)
LEAST = 42


def cost(us):
    return pl.CostEstimate(flops=int(us * 1e6), bytes_accessed=1024, transcendentals=0)


def params(mib):
    return pltpu.CompilerParams(vmem_limit_bytes=mib * 1024 * 1024)


def lane_tiles(ref):
    return [pl.ds(k * LANES, LANES) for k in range(ref.shape[-1] // LANES)]


def block_rows(b):
    return pl.ds(b * LANES, LANES)


def merged_tile(m_ref, s_ref, rows, cols):
    return m_ref[rows, cols] + s_ref[rows, cols].astype(jnp.float32)


def row_scales(own, other):
    inverse = 1.0 / jnp.sqrt(own + other)
    return jnp.broadcast_to(inverse, (LANES, LANES)).T


def head_kernel(first, early, m_hbm, s_hbm, *refs):
    sums_ref, merged_ref = refs[:2]
    m_ref, s_ref, sems = refs[-3:]
    blocks = merged_ref.shape[0] // LANES
    copies = []
    for b in range(blocks):
        there = pl.ds(first + b * LANES, LANES)
        copies.append(pltpu.make_async_copy(m_hbm.at[there], m_ref.at[block_rows(b)], sems.at[2 * b]))
        copies.append(pltpu.make_async_copy(s_hbm.at[there], s_ref.at[block_rows(b)], sems.at[2 * b + 1]))
    for copy in copies:
        copy.start()
    for b in range(blocks):
        copies[2 * b].wait()
        copies[2 * b + 1].wait()
        acc = jnp.zeros((LANES, LANES), jnp.float32)
        for cols in lane_tiles(m_ref):
            v = merged_tile(m_ref, s_ref, block_rows(b), cols)
            merged_ref[block_rows(b), cols] = v
            at = 0
            for early_ref in refs[2 : 2 + len(early)] if b == 0 else ():
                rows = early_ref.shape[0]
                early_ref[:, cols] = v[at : at + rows].astype(jnp.bfloat16)
                at += rows
            acc = acc + v * v
        sums_ref[b] = jnp.sum(acc.T, axis=0, keepdims=True)


def head_norm_kernel(cuts, merged_ref, own_ref, other_ref, *send_refs):
    for (first, count), send_ref in zip(cuts, send_refs, strict=True):
        row = first
        while row < first + count:
            b, skip = row // LANES, row % LANES
            rows = min(LANES - skip, first + count - row)
            inverse = row_scales(own_ref[b], other_ref[b])[skip : skip + rows]
            for cols in lane_tiles(merged_ref):
                v = merged_ref[pl.ds(row, rows), cols] * inverse
                send_ref[pl.ds(row - first, rows), cols] = v.astype(jnp.bfloat16)
            row += rows


def sums_kernel(m_ref, s_ref, *refs):
    sums_ref = refs[-1]
    for b in range(m_ref.shape[0] // LANES):
        acc = jnp.zeros((LANES, LANES), jnp.float32)
        for cols in lane_tiles(m_ref):
            v = merged_tile(m_ref, s_ref, block_rows(b), cols)
            acc = acc + v * v
        sums_ref[b] = jnp.sum(acc.T, axis=0, keepdims=True)


def norm_kernel(m_ref, s_ref, own_ref, other_ref, *refs):
    send_ref, out_ref = refs[-2:]
    for b in range(m_ref.shape[0] // LANES):
        inverse = row_scales(own_ref[b], other_ref[b])
        for cols in lane_tiles(m_ref):
            r = (merged_tile(m_ref, s_ref, block_rows(b), cols) * inverse).astype(jnp.bfloat16)
            send_ref[block_rows(b), cols] = r
            out_ref[block_rows(b), cols] = r


def received_half(out_ref, row, shape):
    rows, width = shape
    side = pl.multiple_of((1 - lax.axis_index("zero")) * width, LANES)
    return out_ref.at[pl.ds(row, rows), pl.ds(side, width)]


def place_kernel(row, recv_ref, _, out_ref, sem):
    copy = pltpu.make_async_copy(recv_ref, received_half(out_ref, row, recv_ref.shape), sem)
    copy.start()
    copy.wait()


def place_early_kernel(row, recv_ref, own_ref, other_ref, _, out_ref, held_ref, sem):
    inverse = row_scales(own_ref[0], other_ref[0])[row : row + recv_ref.shape[0]]
    for cols in lane_tiles(recv_ref):
        held_ref[:, cols] = (recv_ref[:, cols].astype(jnp.float32) * inverse).astype(jnp.bfloat16)
    copy = pltpu.make_async_copy(held_ref, received_half(out_ref, row, recv_ref.shape), sem)
    copy.start()
    copy.wait()


def scale_kernel(inner, *refs):
    out_ref = refs[-1]
    block = 0
    for own_ref, other_ref in zip(refs[:-1:2], refs[1:-1:2], strict=True):
        for b in range(own_ref.shape[0]):
            expert, at = divmod(block * LANES, inner)
            out_ref[pl.ds(expert, 1), pl.ds(at, LANES)] = jnp.sqrt(own_ref[b] + other_ref[b])
            block += 1


def router_rows_kernel(own_ref, other_ref, out_ref):
    width = own_ref.shape[1]
    me = lax.axis_index("zero")
    for ref, at in ((own_ref, me), (other_ref, 1 - me)):
        out_ref[:, pl.ds(pl.multiple_of(at * width, LANES), width)] = ref[...]


def router_kernel(gathered_ref, out_ref):
    devices, columns, _ = gathered_ref.shape
    for d in range(devices):
        out_ref[pl.ds(d * columns, columns), :] = gathered_ref[d]


def in_hbm(x):
    return pltpu.with_memory_space_constraint(x, pltpu.HBM)


def whole_of(m):
    return jax.ShapeDtypeStruct((m.shape[0], 2 * m.shape[1]), jnp.bfloat16)


def sums_shape(blocks):
    return jax.ShapeDtypeStruct((blocks, 1, LANES), jnp.float32)


def head_of(m, s, first, blocks, early, after=()):
    rows, width = blocks * LANES, m.shape[1]
    shapes = [sums_shape(blocks), jax.ShapeDtypeStruct((rows, width), jnp.float32)]
    shapes += [jax.ShapeDtypeStruct((rows, width), jnp.bfloat16) for rows in early]
    return pl.pallas_call(
        after_of(functools.partial(head_kernel, first, early), 2, len(after)),
        in_specs=[ANY, ANY] + [ANY] * len(after),
        out_specs=[VMEM] * len(shapes),
        out_shape=shapes,
        scratch_shapes=[
            pltpu.VMEM((rows, width), m.dtype),
            pltpu.VMEM((rows, width), s.dtype),
            pltpu.SemaphoreType.DMA((2 * blocks,)),
        ],
        compiler_params=params(12),
        cost_estimate=cost(1),
        name="head",
    )(m, s, *after)


def after_of(kernel, at, count):
    def held(*refs):
        return kernel(*refs[:at], *refs[at + count :])

    return held


def head_norm_of(merged, own, other, cuts):
    return pl.pallas_call(
        functools.partial(head_norm_kernel, cuts),
        in_specs=[VMEM] * 3,
        out_specs=[VMEM] * len(cuts),
        out_shape=[jax.ShapeDtypeStruct((count, merged.shape[1]), jnp.bfloat16) for _, count in cuts],
        compiler_params=params(8),
        cost_estimate=cost(1),
        name="head_norm",
    )(merged, own, other)


def scale_of(sums, experts, inner):
    refs = [x for pair in sums for x in pair]
    return pl.pallas_call(
        functools.partial(scale_kernel, inner),
        in_specs=[VMEM] * len(refs),
        out_specs=VMEM,
        out_shape=jax.ShapeDtypeStruct((experts, inner), jnp.float32),
        compiler_params=params(2),
        cost_estimate=cost(1),
        name="scale",
    )(*refs)


def router_rows_of(own, other):
    return pl.pallas_call(
        router_rows_kernel,
        in_specs=[VMEM] * 2,
        out_specs=VMEM,
        out_shape=jax.ShapeDtypeStruct((own.shape[0], 2 * own.shape[1]), own.dtype),
        compiler_params=params(2),
        cost_estimate=cost(1),
        name="router_rows",
    )(own, other)


def router_of(gathered):
    devices, columns, rows = gathered.shape
    return pl.pallas_call(
        router_kernel,
        in_specs=[VMEM],
        out_specs=VMEM,
        out_shape=jax.ShapeDtypeStruct((devices * columns, rows), gathered.dtype),
        compiler_params=params(4),
        cost_estimate=cost(1),
        name="router",
    )(gathered)


def step_rows(*counts):
    for rows in (512, 256):
        if all(count % rows == 0 for count in counts):
            return rows
    return LANES


def sums_of(m, s, first, count, after):
    rows, width = step_rows(first, count), m.shape[1]
    at = first // rows
    block = pl.BlockSpec((rows, width), lambda i: (at + i, 0))
    return pl.pallas_call(
        after_of(sums_kernel, 2, 1),
        grid=(count // rows,),
        in_specs=[block, block, ANY],
        out_specs=pl.BlockSpec((rows // LANES, 1, LANES), lambda i: (i, 0, 0)),
        out_shape=sums_shape(count // LANES),
        compiler_params=params(12),
        cost_estimate=cost(count * 0.002),
        name="sums",
    )(m, s, after)


def norm_of(m, s, own, other, base, first, count, out):
    rows, width = step_rows(first, first - base, count), m.shape[1]
    at, near = first // rows, (first - base) // rows
    block = pl.BlockSpec((rows, width), lambda i: (at + i, 0))
    sums = pl.BlockSpec((rows // LANES, 1, LANES), lambda i: (near + i, 0, 0))
    held = [] if out is None else [out]
    return pl.pallas_call(
        norm_kernel,
        grid=(count // rows,),
        in_specs=[block, block, sums, sums] + [ANY] * len(held),
        out_specs=[
            pl.BlockSpec((rows, width), lambda i: (i, 0)),
            pl.BlockSpec((rows, width), lambda i: (at + i, lax.axis_index("zero"))),
        ],
        out_shape=[jax.ShapeDtypeStruct((count, width), jnp.bfloat16), whole_of(m)],
        input_output_aliases={4: 1} if held else {},
        compiler_params=params(14),
        cost_estimate=cost(count * 0.003),
        name="norm",
    )(m, s, own, other, *held)


def place(recv, out, row):
    return pl.pallas_call(
        functools.partial(place_kernel, row),
        in_specs=[VMEM, ANY],
        out_specs=ANY,
        out_shape=jax.ShapeDtypeStruct(out.shape, out.dtype),
        scratch_shapes=[pltpu.SemaphoreType.DMA],
        input_output_aliases={1: 0},
        compiler_params=params(6),
        cost_estimate=cost(1),
        name="place",
    )(recv, out)


def place_early(recv, own, other, out, row):
    return pl.pallas_call(
        functools.partial(place_early_kernel, row),
        in_specs=[VMEM, VMEM, VMEM, ANY],
        out_specs=ANY,
        out_shape=jax.ShapeDtypeStruct(out.shape, out.dtype),
        scratch_shapes=[pltpu.VMEM(recv.shape, jnp.bfloat16), pltpu.SemaphoreType.DMA],
        input_output_aliases={3: 0},
        compiler_params=params(2),
        cost_estimate=cost(1),
        name="place_early",
    )(recv, own, other, out)


def swap(x):
    return lax.ppermute(x, "zero", PAIR)


def long_cuts(blocks):
    sizes = []
    while blocks > LONG + 4:
        sizes.append(LONG)
        blocks -= LONG
    while blocks > 1:
        sizes.append((blocks + 1) // 2)
        blocks //= 2
    return sizes + [1] * blocks


def pair_steps(master_down, second_down, router_weight, router_gain):
    experts, inner, width = master_down.shape
    n = experts * inner
    m, s = in_hbm(master_down.reshape(n, width)), in_hbm(second_down.reshape(n, width))
    head, near = HEAD * LANES, (HEAD + NEXT) * LANES
    recvs = []

    own0, merged0, *early = head_of(m, s, 0, HEAD, PARTS)
    other_early = [swap(x) for x in early]
    sums0 = own0, swap(own0)
    half = EARLY + (head - EARLY) * 2 // 3 // 16 * 16
    send_a, send_b = head_norm_of(merged0, *sums0, ((EARLY, half - EARLY), (half, head - half)))
    recvs.append((EARLY, swap(send_a)))
    own1, merged1 = head_of(m, s, head, NEXT, (), (send_a,))
    sums1 = own1, swap(own1)
    recvs.append((half, swap(send_b)))

    half = (NEXT + 1) // 2 * LANES
    (send_a,) = head_norm_of(merged1, *sums1, ((0, half),))
    recvs.append((head, swap(send_a)))
    own2 = sums_of(m, s, near, n - near, send_a)
    sums2 = own2, swap(own2)
    (send_b,) = head_norm_of(merged1, *sums1, ((half, NEXT * LANES - half),))
    recvs.append((head + half, swap(send_b)))
    part_router = (router_weight.T * router_gain).astype(jnp.bfloat16)
    other_router = swap(part_router)

    rows = router_rows_of(part_router, other_router)
    serve_router = router_of(lax.all_gather(rows, "bank")).T

    def ready(out, ahead):
        if recvs[0][0] == EARLY:
            _, out = norm_of(m, s, *sums0, 0, 0, head, out)
            _, out = norm_of(m, s, *sums1, head, head, near - head, out)
            at = 0
            for recv in other_early:
                out = place_early(recv, *sums0, out, at)
                at += recv.shape[0]
        while recvs and sum(recv.shape[0] for _, recv in recvs[1:]) >= ahead:
            at, recv = recvs.pop(0)
            out = place(recv, out, at)
        return out

    out, row, label = None, near, 4
    for size in long_cuts(n // LANES - HEAD - NEXT - 1):
        if label > 5:
            out = ready(out, AHEAD * LANES)
        send, out = norm_of(m, s, *sums2, near, row, size * LANES, out)
        recvs.append((row, swap(send)))
        row += size * LANES
        label += 1
    cuts, at = [], 0
    for rows in LAST:
        cuts.append((at, rows))
        at += rows
    _, merged = head_of(m, s, n - LANES, 1, (), (send,))
    sends = head_norm_of(merged, *(x[-1:] for x in sums2), tuple(cuts))
    for (at, _), send in zip(cuts, sends, strict=True):
        recvs.append((n - LANES + at, swap(send)))
        label += 1
    _, out = norm_of(m, s, *sums2, near, n - LANES, LANES, out)
    scale_down = scale_of((sums0, sums1, sums2), experts, inner)
    out = ready(out, 0)
    return out.reshape(experts, inner, 2 * width), scale_down, serve_router


def gather_body(master_down, second_down, router_weight, router_gain):
    merged_down = master_down + second_down.astype(jnp.float32)
    total_down = lax.psum(jnp.sum(merged_down * merged_down, axis=2), "zero")
    scale_down = jnp.sqrt(total_down)
    narrow_down = (merged_down / jnp.expand_dims(scale_down, 2)).astype(jnp.bfloat16)
    final_down = lax.all_gather(narrow_down, "zero", axis=2, tiled=True)
    part_router = (router_weight * router_gain[:, None]).astype(jnp.bfloat16)
    row_router = lax.all_gather(part_router, "zero", axis=0, tiled=True)
    serve_router = lax.all_gather(row_router, "bank", axis=1, tiled=True)
    return (final_down, scale_down, serve_router)


def solution(mesh):
    specs = dict(
        mesh=mesh,
        in_specs=(P("bank", None, "zero"), P("bank", None, "zero"), P("zero", "bank"), P("zero")),
        out_specs=(P("bank", None, None), P("bank", None), P()),
        check_vma=False,
    )
    general = jax.shard_map(gather_body, **specs)

    def step(master_down, *rest):
        experts, inner, width = master_down.shape
        blocks, over = divmod(experts // mesh.shape["bank"] * inner, LANES)
        if mesh.shape["zero"] != 2 or over or blocks < LEAST or inner % LANES or width % LANES:
            return general(master_down, *rest)
        return jax.shard_map(pair_steps, **specs)(master_down, *rest)

    return step
```
